32 devices in a mesh: data: 32 (over z, y, x, core).
Axes of the slice: x: 2, y: 2, z: 4, core: 2. Of those that a mesh axis runs over, the one named last changes fastest.
Arguments:
- feat_img: bfloat16 [16384, 2048], P('data')
- feat_txt: bfloat16 [16384, 512], P('data')
- w_img: bfloat16 [2048, 1024], replicated
- w_txt: bfloat16 [512, 1024], replicated
- log_temp: float32 [], replicated
- logit_bias: float32 [], replicated
- pair_ids: int32 [16384], P('data')
Outputs:
- output 1: float32 [], replicated
- output 2: float32 [], replicated
- output 3: float32 [], replicated
- output 4: float32 [2048, 1024], replicated
- output 5: float32 [512, 1024], replicated
All inputs are finite; a program needn't handle non-finite values.
Results may differ from the reference program's by a relative error of at most 0.001.
Values are sent between devices in bfloat16 or wider.
A program may use at most 1 GiB of HBM per device.

```python
import jax
import jax.numpy as jnp
from jax import lax

ROWS_DEV = 512
DEVICES = 32
EMBED = 1024
FEAT_IMG = 2048
FEAT_TXT = 512
LATENT = 16

BATCH = ROWS_DEV * DEVICES


def feature_draw(base_key, feat_width):
    key_list = jax.random.split(base_key, 4)
    latents = jax.random.normal(key_list[0], (BATCH, LATENT), jnp.float32)
    basis_rows = jax.random.normal(key_list[1], (LATENT, feat_width), jnp.float32)
    center = jax.random.normal(key_list[2], (feat_width,), jnp.float32)
    noise_rows = jax.random.normal(key_list[3], (BATCH, feat_width), jnp.float32)
    feat_out = center + jnp.dot(latents, basis_rows) * LATENT ** -0.5 + 0.5 * noise_rows
    return feat_out.astype(jnp.bfloat16)


def setup_inputs(seed: int = 0) -> dict:
    key_list = jax.random.split(jax.random.key(seed), 7)
    w_img = jax.random.normal(key_list[2], (FEAT_IMG, EMBED), jnp.float32) * FEAT_IMG ** -0.5
    w_txt = jax.random.normal(key_list[3], (FEAT_TXT, EMBED), jnp.float32) * FEAT_TXT ** -0.5
    log_temp = jnp.log(10.0) + jax.random.uniform(key_list[4], (), jnp.float32, -0.5, 0.5)
    logit_bias = -jnp.log(float(BATCH)) + jax.random.uniform(key_list[5], (), jnp.float32, -0.5, 1.5)
    pair_ids = (jax.random.permutation(key_list[6], BATCH) // 2).astype(jnp.int32)
    return {
        "feat_img": feature_draw(key_list[0], FEAT_IMG),
        "feat_txt": feature_draw(key_list[1], FEAT_TXT),
        "w_img": w_img.astype(jnp.bfloat16),
        "w_txt": w_txt.astype(jnp.bfloat16),
        "log_temp": log_temp.astype(jnp.float32),
        "logit_bias": logit_bias.astype(jnp.float32),
        "pair_ids": pair_ids,
    }


def reference(feat_img, feat_txt, w_img, w_txt, log_temp, logit_bias, pair_ids):
    temp_scale = jnp.exp(log_temp)
    raw_img = jnp.dot(feat_img, w_img, preferred_element_type=jnp.float32)
    raw_txt = jnp.dot(feat_txt, w_txt, preferred_element_type=jnp.float32)
    inv_img = lax.rsqrt(jnp.sum(raw_img * raw_img, axis=1, keepdims=True))
    inv_txt = lax.rsqrt(jnp.sum(raw_txt * raw_txt, axis=1, keepdims=True))
    unit_img = raw_img * inv_img
    unit_txt = raw_txt * inv_txt
    emb_img = unit_img.astype(jnp.bfloat16)
    emb_txt = unit_txt.astype(jnp.bfloat16)

    def row_block(loop_state, block_in):
        acc_txt, loss_sum, temp_sum, bias_sum = loop_state
        emb_blk, ids_blk = block_in
        sim_tile = jnp.dot(emb_blk, emb_txt.T, preferred_element_type=jnp.float32)
        label_sign = jnp.where(ids_blk[:, None] == pair_ids[None, :], 1.0, -1.0).astype(jnp.float32)
        margin = -label_sign * (temp_scale * sim_tile + logit_bias)
        grad_tile = -label_sign * jax.nn.sigmoid(margin) / BATCH
        grad_bf = grad_tile.astype(jnp.bfloat16)
        grad_blk = jnp.dot(grad_bf, emb_txt, preferred_element_type=jnp.float32)
        acc_txt = acc_txt + jnp.dot(grad_bf.T, emb_blk, preferred_element_type=jnp.float32)
        new_state = (
            acc_txt,
            loss_sum + jnp.sum(jax.nn.softplus(margin)),
            temp_sum + jnp.sum(grad_tile * sim_tile),
            bias_sum + jnp.sum(grad_tile),
        )
        return new_state, grad_blk

    zero_sum = jnp.zeros((), jnp.float32)
    init_state = (jnp.zeros((BATCH, EMBED), jnp.float32), zero_sum, zero_sum, zero_sum)
    block_in = (emb_img.reshape(DEVICES, ROWS_DEV, EMBED), pair_ids.reshape(DEVICES, ROWS_DEV))
    final_state, grad_blocks = lax.scan(row_block, init_state, block_in)
    acc_txt, loss_sum, temp_sum, bias_sum = final_state
    grad_img = temp_scale * grad_blocks.reshape(BATCH, EMBED)
    grad_txt = temp_scale * acc_txt
    raw_grad_img = inv_img * (grad_img - unit_img * jnp.sum(unit_img * grad_img, axis=1, keepdims=True))
    raw_grad_txt = inv_txt * (grad_txt - unit_txt * jnp.sum(unit_txt * grad_txt, axis=1, keepdims=True))
    grad_w_img = jnp.dot(feat_img.T, raw_grad_img.astype(jnp.bfloat16), preferred_element_type=jnp.float32)
    grad_w_txt = jnp.dot(feat_txt.T, raw_grad_txt.astype(jnp.bfloat16), preferred_element_type=jnp.float32)
    return loss_sum / BATCH, temp_scale * temp_sum, bias_sum, grad_w_img, grad_w_txt
```

```python
import functools

import jax
import jax.numpy as jnp
from jax import lax
from jax.experimental import pallas as pl
from jax.experimental.pallas import tpu as pltpu
from jax.sharding import PartitionSpec as P

CONTRACT_ROWS = (((0,), (0,)), ((), ()))
CONTRACT_COLS = (((1,), (1,)), ((), ()))
LOG2E = 1.4426950408889634
LN2 = 0.6931471805599453
ROW_CHUNK = 256
COL_CHUNK = 256


def embed_rows(feat_rows, weights):
    raw_emb = jnp.dot(feat_rows, weights, preferred_element_type=jnp.float32)
    inv_norm = lax.rsqrt(jnp.sum(raw_emb * raw_emb, axis=1, keepdims=True))
    unit_emb = raw_emb * inv_norm
    return unit_emb, inv_norm, unit_emb.astype(jnp.bfloat16)


def weight_grad(feat_rows, unit_emb, inv_norm, grad_emb):
    raw_grad = inv_norm * (grad_emb - unit_emb * jnp.sum(unit_emb * grad_emb, axis=1, keepdims=True))
    return lax.dot_general(feat_rows, raw_grad.astype(jnp.bfloat16), CONTRACT_ROWS, preferred_element_type=jnp.float32)


def log1p_sum(expo):
    terms = [expo[8 * k:8 * k + 8] for k in range(expo.shape[0] // 8)]
    while len(terms) > 1:
        terms = [terms[2 * k] + terms[2 * k + 1] + terms[2 * k] * terms[2 * k + 1] for k in range(len(terms) // 2)]
    prod = terms[0]
    one_plus = 1.0 + prod
    return jnp.log(one_plus) + (prod - (one_plus - 1.0)) / one_plus


def fold_rows(tile):
    terms = [tile[8 * k:8 * k + 8] for k in range(tile.shape[0] // 8)]
    while len(terms) > 1:
        terms = [terms[2 * k] + terms[2 * k + 1] for k in range(len(terms) // 2)]
    return terms[0]


AXES = {"c": (2, 1), "x": (2, 2), "y": (2, 4), "z": (4, 8)}
MESH_ID = pl.DeviceIdType.MESH


def coordinate(me, axis):
    size, stride = AXES[axis]
    return lax.rem(lax.div(me, stride), size)


def peer_of(me, axis, dist):
    size, stride = AXES[axis]
    here = coordinate(me, axis)
    return me + (lax.rem(here + dist, size) - here) * stride


def rows_at(start, size):
    return pl.ds(pl.multiple_of(start, 8), size)


class Slab:
    def __init__(self, src, dst, row0, rows, order):
        self.src, self.dst, self.row0, self.rows, self.order = src, dst, row0, rows, order

    def piece(self, stage):
        rows = self.rows
        for axis in self.order[:stage + 1]:
            rows //= AXES[axis][0]
        return rows


def sum_plan(wi_rows, wt_rows, sub):
    plan = []
    for k in range(sub):
        half = wi_rows // 2 // sub
        part = wt_rows // sub
        plan.append((0, k * half, half, "cxyz"))
        plan.append((0, wi_rows // 2 + k * half, half, "cyxz"))
        plan.append((1, k * part, part, "czxy"))
    plan.append((2, 0, 256, "cxyz"))
    return plan


def sum_kernel(plan, *refs):
    ins, outs = refs[:3], refs[3:6]
    n = len(plan)
    held = refs[6:6 + n]
    land = refs[6 + n:6 + 5 * n]
    send_sem, recv_sem = refs[6 + 5 * n:]
    me = lax.axis_index("data")
    slabs = [Slab(ins[a], outs[a], row0, rows, order) for a, row0, rows, order in plan]

    barrier = pltpu.get_barrier_semaphore()
    partners = [peer_of(me, axis, d) for axis in "cxyz" for d in range(1, AXES[axis][0])]
    for dev in partners:
        pl.semaphore_signal(barrier, inc=1, device_id=(dev,), device_id_type=MESH_ID)
    pl.semaphore_wait(barrier, len(partners))

    counter = [0]
    started = []

    def send(src, dst, dev):
        k = counter[0]
        counter[0] += 1
        copy = pltpu.make_async_remote_copy(
            src_ref=src, dst_ref=dst, send_sem=send_sem.at[k], recv_sem=recv_sem.at[k],
            device_id=(dev,), device_id_type=MESH_ID)
        copy.start()
        started.append(copy)
        return copy

    offs = [0] * n
    pending = [None] * n

    def scatter(i, stage):
        slab = slabs[i]
        axis = slab.order[stage]
        size = AXES[axis][0]
        piece = slab.piece(stage)
        here = coordinate(me, axis)
        copies = []
        for d in range(1, size):
            there = lax.rem(here + d, size)
            if stage == 0:
                src = slab.src.at[rows_at(slab.row0 + there * piece, piece)]
            else:
                src = held[i].at[rows_at(offs[i] + there * piece, piece)]
            copies.append(send(src, land[4 * i + stage].at[d - 1], peer_of(me, axis, d)))
        pending[i] = copies

    def absorb(i, stage):
        slab = slabs[i]
        axis = slab.order[stage]
        piece = slab.piece(stage)
        here = coordinate(me, axis)
        for copy in pending[i]:
            copy.wait_recv()
        base = offs[i] + here * piece
        step = min(piece, 32)

        def add(k, _):
            at = k * step
            if stage == 0:
                total = slab.src[rows_at(slab.row0 + base + at, step), :]
            else:
                total = held[i][rows_at(base + at, step), :]
            for d in range(AXES[axis][0] - 1):
                total = total + land[4 * i + stage][d, rows_at(at, step), :]
            if stage == 0:
                held[i][rows_at(at, step), :] = total
            elif stage == 3:
                slab.dst[rows_at(slab.row0 + home[i] + at, step), :] = total
            else:
                held[i][rows_at(base + at, step), :] = total
            return 0

        if stage == 0:
            home[i] = here * piece
        else:
            home[i] = home[i] + here * piece
        lax.fori_loop(0, piece // step, add, 0)
        offs[i] = 0 if stage == 0 else base

    home = [0] * n

    for i in range(n):
        scatter(i, 0)
    for stage in range(4):
        for i in range(n):
            absorb(i, stage)
            if stage < 3:
                scatter(i, stage + 1)
            else:
                spread(i, 3, slabs, home, me, send, pending)
    for stage in (2, 1, 0):
        for i in range(n):
            for copy in pending[i]:
                copy.wait_recv()
            here = coordinate(me, slabs[i].order[stage + 1])
            home[i] = home[i] - here * slabs[i].piece(stage + 1)
            spread(i, stage, slabs, home, me, send, pending)
    for i in range(n):
        for copy in pending[i]:
            copy.wait_recv()
    for copy in started:
        copy.wait_send()


def spread(i, stage, slabs, home, me, send, pending):
    slab = slabs[i]
    axis = slab.order[stage]
    piece = slab.piece(stage)
    view = slab.dst.at[rows_at(slab.row0 + home[i], piece)]
    pending[i] = [send(view, view, peer_of(me, axis, d)) for d in range(1, AXES[axis][0])]


def sum_over_devices(dw_img, dw_txt, small, sub=2):
    plan = sum_plan(dw_img.shape[0], dw_txt.shape[0], sub)
    arrays = [dw_img, dw_txt, small]
    held, land = [], []
    copies = 0
    for a, _, rows, order in plan:
        width = arrays[a].shape[1]
        slab = Slab(None, None, 0, rows, order)
        held.append(pltpu.VMEM((slab.piece(0), width), jnp.float32))
        for stage in range(4):
            others = AXES[order[stage]][0] - 1
            land.append(pltpu.VMEM((others, slab.piece(stage), width), jnp.float32))
            copies += 2 * others
    return pl.pallas_call(
        functools.partial(sum_kernel, plan),
        out_shape=[jax.ShapeDtypeStruct(a.shape, jnp.float32) for a in arrays],
        in_specs=[pl.BlockSpec(memory_space=pltpu.VMEM)] * 3,
        out_specs=[pl.BlockSpec(memory_space=pltpu.VMEM)] * 3,
        scratch_shapes=held + land + [pltpu.SemaphoreType.DMA((copies,)), pltpu.SemaphoreType.DMA((copies,))],
        compiler_params=pltpu.CompilerParams(
            collective_id=1, has_side_effects=True, vmem_limit_bytes=60 * 1024 * 1024),
    )(*arrays)


ID_ROWS = 16


def with_ids(block, ids):
    rows, width = block.shape
    digits = jnp.stack([lax.div(ids, 128), lax.rem(ids, 128)]).astype(jnp.bfloat16)
    digits = jnp.pad(digits, ((0, ID_ROWS - 2), (0, width - rows)))
    return jnp.concatenate([block, digits], axis=0)


def cross_kernel(scal_ref, img_in, txt_in, w_ref, img_out, txt_out, sums_ref,
                 img_all, txt_all, own_txt, emb, grad_ref, rid_img, rid_txt, acc_img, acc_txt, land_img, land_txt,
                 img_send, img_recv, txt_send, txt_recv, swap_send, swap_recv, copy_sem):
    rows = own_txt.shape[1]
    me = lax.axis_index("data")
    core, col_x, col_y, lev = (coordinate(me, a) for a in "cxyz")
    scale = scal_ref[0]
    bias = scal_ref[1]

    load_img = pltpu.make_async_copy(img_in, img_all.at[lev * 4 + col_x * 2 + core], copy_sem.at[0])
    load_txt = pltpu.make_async_copy(txt_in, txt_all.at[lev * 4 + col_y * 2 + core], copy_sem.at[1])
    load_img.start()
    load_txt.start()

    barrier = pltpu.get_barrier_semaphore()
    for axis in "cxy":
        pl.semaphore_signal(barrier, inc=1, device_id=(peer_of(me, axis, 1),), device_id_type=MESH_ID)

    @pl.when(lev > 0)
    def _():
        pl.semaphore_signal(barrier, inc=1, device_id=(me - 8,), device_id_type=MESH_ID)

    @pl.when(lev < 3)
    def _():
        pl.semaphore_signal(barrier, inc=1, device_id=(me + 8,), device_id_type=MESH_ID)

    pl.semaphore_wait(barrier, 3 + jnp.where(lev > 0, 1, 0) + jnp.where(lev < 3, 1, 0))

    class Stream:
        def __init__(self, buf, send_sem, recv_sem, axis):
            self.buf, self.send_sem, self.recv_sem, self.axis = buf, send_sem, recv_sem, axis
            self.side = coordinate(me, axis)
            self.peers = (me + 8, me - 8, peer_of(me, axis, 1), peer_of(me, "c", 1))

        def slot(self, level, near, same_core):
            side = jnp.where(near, self.side, 1 - self.side)
            return level * 4 + side * 2 + jnp.where(same_core, core, 1 - core)

        def copy(self, slot, target):
            return pltpu.make_async_remote_copy(
                src_ref=self.buf.at[slot], dst_ref=self.buf.at[slot],
                send_sem=self.send_sem.at[slot * 4 + target], recv_sem=self.recv_sem.at[slot],
                device_id=(self.peers[target],), device_id_type=MESH_ID)

        def each_target(self, level, near, act):
            slot = self.slot(level, near, True)
            if near:
                @pl.when((level <= lev) & (lev < 3))
                def _():
                    act(self.copy(slot, 0))

                @pl.when((level >= lev) & (lev > 0))
                def _():
                    act(self.copy(slot, 1))

                act(self.copy(slot, 2))
            act(self.copy(slot, 3))

        def arrive(self, level, near, same_core):
            self.copy(self.slot(level, near, same_core), 3).wait_recv()

        def relay(self, dist, near):
            for sign in (-1, 1):
                level = lev + sign * dist
                valid = (level >= 0) & (level <= 3)
                if sign == -1:
                    valid = valid & (dist > 0)

                @pl.when(valid)
                def _():
                    if near:
                        @pl.when(dist > 0)
                        def _():
                            self.arrive(level, True, True)
                    else:
                        self.arrive(level, False, True)
                    self.each_target(level, near, lambda c: c.start())

    txt = Stream(txt_all, txt_send, txt_recv, "y")
    img = Stream(img_all, img_send, img_recv, "x")

    load_txt.wait()
    txt.relay(0, True)
    load_img.wait()
    img.relay(0, True)

    sums_ref[...] = jnp.zeros_like(sums_ref)
    acc_img[...] = jnp.zeros_like(acc_img)
    acc_txt[...] = jnp.zeros_like(acc_txt)

    def id_row(buf, slot):
        digits = buf[slot, pl.ds(rows, ID_ROWS), pl.ds(0, rows)].astype(jnp.float32)
        return digits[0:1] * 128.0 + digits[1:2]

    def id_tile(buf, slot):
        return jnp.transpose(jnp.broadcast_to(id_row(buf, slot), (COL_CHUNK, rows)))

    def embed_block(slot, dst):
        for cc in range(rows // COL_CHUNK):
            sl = pl.ds(cc * COL_CHUNK, COL_CHUNK)
            raw = jnp.dot(txt_all[slot, sl, :], w_ref[...], preferred_element_type=jnp.float32)
            inv = lax.rsqrt(jnp.sum(raw * raw, axis=1, keepdims=True))
            dst[sl, :] = (raw * inv).astype(jnp.bfloat16)

    def block_pass(row_view, rid, acc, col_view, cid, with_loss):
        for half in range(2):
            for rc in range(rows // ROW_CHUNK):
                rsl = pl.ds(rc * ROW_CHUNK, ROW_CHUNK)
                gsl = pl.ds(half * rows + rc * ROW_CHUNK, ROW_CHUNK)
                for cc in range(rows // COL_CHUNK):
                    csl = pl.ds(cc * COL_CHUNK, COL_CHUNK)
                    sim = lax.dot_general(row_view(half)[rsl, :], col_view[csl, :], CONTRACT_COLS,
                                          preferred_element_type=jnp.float32)
                    match = rid[half, rsl, :] == cid[:, cc * COL_CHUNK:(cc + 1) * COL_CHUNK]
                    margin = sim * scale + bias
                    margin = jnp.where(match, -margin, margin)
                    if with_loss:
                        expo = jnp.exp2(-jnp.abs(margin))
                        recip = 1.0 / (1.0 + expo)
                        sig = jnp.where(margin >= 0.0, recip, expo * recip)
                        grad = jnp.where(match, -sig, sig)
                        sums_ref[0] += fold_rows(jnp.maximum(margin, 0.0))
                        sums_ref[1] += log1p_sum(expo)
                        sums_ref[2] += fold_rows(grad * sim)
                        sums_ref[3] += fold_rows(grad)
                    else:
                        sig = 1.0 / (1.0 + jnp.exp2(-margin))
                        grad = jnp.where(match, -sig, sig)
                    grad_ref[gsl, csl] = grad.astype(jnp.bfloat16)
                acc[half, rsl, :] += jnp.dot(grad_ref[gsl, :], col_view[pl.ds(0, rows), :],
                                             preferred_element_type=jnp.float32)

    own_slots = [img.slot(lev, True, True), img.slot(lev, False, True)]
    txt_slots = [txt.slot(lev, True, True), txt.slot(lev, False, True)]

    def level_at(k):
        inner = (lev == 1) | (lev == 2)
        near_low = jnp.where(inner & (k < 2), 1 - k, k)
        return jnp.where(lev >= 2, 3 - near_low, near_low)

    def round_body(k, _):
        level = level_at(k)

        @pl.when(k > 0)
        def _():
            txt.relay(k, True)

        def run_txt(j, _):
            near = j < 2
            same = lax.rem(j, 2) == 0

            @pl.when(j == 0)
            def _():
                @pl.when(k == 0)
                def _():
                    img.relay(0, False)
                    txt.relay(0, False)
                    embed_block(txt_slots[0], own_txt.at[0])
                    embed_block(txt_slots[1], own_txt.at[1])
                    for half in range(2):
                        rid_img[half] = id_tile(img_all, own_slots[half])
                        rid_txt[half] = id_tile(txt_all, txt_slots[half])

            @pl.when(j == 2)
            def _():
                @pl.when(k > 0)
                def _():
                    img.relay(k, True)
                    txt.relay(k, False)

            @pl.when(jnp.logical_not(same))
            def _():
                txt.arrive(level, near, False)

            slot = txt.slot(level, near, same)
            embed_block(slot, emb)
            block_pass(lambda half: img_all.at[own_slots[half]], rid_img, acc_img, emb, id_row(txt_all, slot), True)
            return 0

        lax.fori_loop(0, 4, run_txt, 0)

        def run_img(j, _):
            near = j < 2
            same = lax.rem(j, 2) == 0

            @pl.when((j == 2) & (k > 0))
            def _():
                img.relay(k, False)

            @pl.when(jnp.logical_not(same))
            def _():
                img.arrive(level, near, False)

            slot = img.slot(level, near, same)
            block_pass(lambda half: own_txt.at[half], rid_txt, acc_txt, img_all.at[slot], id_row(img_all, slot), False)
            return 0

        @pl.when(k == 3)
        def _():
            swap(acc_img, land_img, "x", 0).start()

        lax.fori_loop(0, 4, run_img, 0)
        return 0

    def swap(acc, land, axis, k):
        return pltpu.make_async_remote_copy(
            src_ref=acc.at[1], dst_ref=land, send_sem=swap_send.at[k], recv_sem=swap_recv.at[k],
            device_id=(peer_of(me, axis, 1),), device_id_type=MESH_ID)

    lax.fori_loop(0, 4, round_body, 0)

    swap_img = swap(acc_img, land_img, "x", 0)
    swap_txt = swap(acc_txt, land_txt, "y", 1)
    swap_txt.start()

    def settle(level, _):
        for stream in (txt, img):
            for near in (True, False):
                stream.each_target(level, near, lambda c: c.wait_send())
        return 0

    lax.fori_loop(0, 4, settle, 0)
    swap_img.wait()
    img_out[...] = acc_img[0] + land_img[...]
    swap_txt.wait()
    txt_out[...] = acc_txt[0] + land_txt[...]


def cross_pass(scalars, img_block, txt_block, w_txt):
    rows, emb = img_block.shape[0] - ID_ROWS, img_block.shape[1]
    width = txt_block.shape[1]
    full = rows + ID_ROWS
    f32, bf16 = jnp.float32, jnp.bfloat16
    dma = pltpu.SemaphoreType.DMA
    return pl.pallas_call(
        cross_kernel,
        out_shape=[jax.ShapeDtypeStruct((rows, emb), f32), jax.ShapeDtypeStruct((rows, emb), f32),
                   jax.ShapeDtypeStruct((4, 8, COL_CHUNK), f32)],
        in_specs=[pl.BlockSpec(memory_space=pltpu.SMEM), pl.BlockSpec(memory_space=pl.ANY),
                  pl.BlockSpec(memory_space=pl.ANY), pl.BlockSpec(memory_space=pltpu.VMEM)],
        out_specs=[pl.BlockSpec(memory_space=pltpu.VMEM)] * 3,
        scratch_shapes=[
            pltpu.VMEM((16, full, emb), bf16), pltpu.VMEM((16, full, width), bf16),
            pltpu.VMEM((2, rows, emb), bf16), pltpu.VMEM((rows, emb), bf16), pltpu.VMEM((2 * rows, rows), bf16),
            pltpu.VMEM((2, rows, COL_CHUNK), f32), pltpu.VMEM((2, rows, COL_CHUNK), f32),
            pltpu.VMEM((2, rows, emb), f32), pltpu.VMEM((2, rows, emb), f32),
            pltpu.VMEM((rows, emb), f32), pltpu.VMEM((rows, emb), f32),
            dma((64,)), dma((16,)), dma((64,)), dma((16,)), dma((2,)), dma((2,)), dma((2,)),
        ],
        compiler_params=pltpu.CompilerParams(
            collective_id=0, has_side_effects=True, vmem_limit_bytes=62 * 1024 * 1024),
    )(scalars, img_block, txt_block, w_txt)


def solution(mesh):
    n_dev = mesh.shape["data"]

    def local_fn(feat_img, feat_txt, w_img, w_txt, log_temp, logit_bias, pair_ids):
        total_rows = feat_img.shape[0] * n_dev
        temp_scale = jnp.exp(log_temp)
        scalars = jnp.stack([temp_scale * LOG2E, logit_bias * LOG2E])
        unit_img, inv_img, emb_img = embed_rows(feat_img, w_img)
        unit_txt, inv_txt, _ = embed_rows(feat_txt, w_txt)
        acc_img, acc_txt, sums = cross_pass(scalars, with_ids(emb_img, pair_ids), with_ids(feat_txt, pair_ids), w_txt)
        out_scale = temp_scale / total_rows
        dw_img = weight_grad(feat_img, unit_img, inv_img, out_scale * acc_img)
        dw_txt = weight_grad(feat_txt, unit_txt, inv_txt, out_scale * acc_txt)
        sums = jnp.sum(sums, axis=(1, 2))
        small = jnp.stack([LN2 * sums[0] + sums[1], sums[2], sums[3]]) / total_rows
        small = jnp.pad(small[:, None], ((0, 253), (0, 127)))
        dw_img, dw_txt, small = sum_over_devices(dw_img, dw_txt, small)
        return small[0, 0], temp_scale * small[1, 0], small[2, 0], dw_img, dw_txt

    return jax.shard_map(
        local_fn,
        mesh=mesh,
        in_specs=(P("data", None), P("data", None), P(None, None), P(None, None), P(), P(), P("data")),
        out_specs=(P(), P(), P(), P(None, None), P(None, None)),
        check_vma=False,
    )
```

```python
import functools

import jax
import jax.numpy as jnp
from jax import lax
from jax.experimental import pallas as pl
from jax.experimental.pallas import tpu as pltpu
from jax.sharding import PartitionSpec as P

CONTRACT_ROWS = (((0,), (0,)), ((), ()))
CONTRACT_COLS = (((1,), (1,)), ((), ()))
LOG2E = 1.4426950408889634
LN2 = 0.6931471805599453
COL_CHUNK = 256


def embed_rows(feat_rows, weights):
    raw_emb = jnp.dot(feat_rows, weights, preferred_element_type=jnp.float32)
    inv_norm = lax.rsqrt(jnp.sum(raw_emb * raw_emb, axis=1, keepdims=True))
    unit_emb = raw_emb * inv_norm
    return unit_emb, inv_norm, unit_emb.astype(jnp.bfloat16)


def weight_grad(feat_rows, unit_emb, inv_norm, grad_emb):
    raw_grad = inv_norm * (grad_emb - unit_emb * jnp.sum(unit_emb * grad_emb, axis=1, keepdims=True))
    return lax.dot_general(feat_rows, raw_grad.astype(jnp.bfloat16), CONTRACT_ROWS, preferred_element_type=jnp.float32)


def log1p_sum(expo):
    terms = [expo[8 * k:8 * k + 8] for k in range(expo.shape[0] // 8)]
    while len(terms) > 1:
        terms = [terms[2 * k] + terms[2 * k + 1] + terms[2 * k] * terms[2 * k + 1] for k in range(len(terms) // 2)]
    prod = terms[0]
    one_plus = 1.0 + prod
    return jnp.log(one_plus) + (prod - (one_plus - 1.0)) / one_plus


def fold_rows(tile):
    terms = [tile[8 * k:8 * k + 8] for k in range(tile.shape[0] // 8)]
    while len(terms) > 1:
        terms = [terms[2 * k] + terms[2 * k + 1] for k in range(len(terms) // 2)]
    return terms[0]


AXES = {"c": (2, 1), "x": (2, 2), "y": (2, 4), "z": (4, 8)}
MESH_ID = pl.DeviceIdType.MESH


def coordinate(me, axis):
    size, stride = AXES[axis]
    return lax.rem(lax.div(me, stride), size)


def peer_of(me, axis, dist):
    size, stride = AXES[axis]
    here = coordinate(me, axis)
    return me + (lax.rem(here + dist, size) - here) * stride


def rows_at(start, size):
    return pl.ds(pl.multiple_of(start, 8), size)


class Slab:
    def __init__(self, src, dst, row0, rows, order):
        self.src, self.dst, self.row0, self.rows, self.order = src, dst, row0, rows, order

    def piece(self, stage):
        rows = self.rows
        for axis in self.order[:stage + 1]:
            rows //= AXES[axis][0]
        return rows


def sum_plan(wi_rows, wt_rows, sub):
    plan = []
    for k in range(sub):
        half = wi_rows // 2 // sub
        part = wt_rows // sub
        plan.append((0, k * half, half, "cxyz"))
        plan.append((0, wi_rows // 2 + k * half, half, "cyxz"))
        plan.append((1, k * part, part, "czxy"))
    plan.append((2, 0, 256, "cxyz"))
    return plan


def sum_kernel(plan, *refs):
    ins, outs = refs[:3], refs[3:6]
    n = len(plan)
    held = refs[6:6 + n]
    land = refs[6 + n:6 + 5 * n]
    send_sem, recv_sem = refs[6 + 5 * n:]
    me = lax.axis_index("data")
    slabs = [Slab(ins[a], outs[a], row0, rows, order) for a, row0, rows, order in plan]

    barrier = pltpu.get_barrier_semaphore()
    partners = [peer_of(me, axis, d) for axis in "cxyz" for d in range(1, AXES[axis][0])]
    for dev in partners:
        pl.semaphore_signal(barrier, inc=1, device_id=(dev,), device_id_type=MESH_ID)
    pl.semaphore_wait(barrier, len(partners))

    counter = [0]
    started = []

    def send(src, dst, dev):
        k = counter[0]
        counter[0] += 1
        copy = pltpu.make_async_remote_copy(
            src_ref=src, dst_ref=dst, send_sem=send_sem.at[k], recv_sem=recv_sem.at[k],
            device_id=(dev,), device_id_type=MESH_ID)
        copy.start()
        started.append(copy)
        return copy

    offs = [0] * n
    pending = [None] * n

    def scatter(i, stage):
        slab = slabs[i]
        axis = slab.order[stage]
        size = AXES[axis][0]
        piece = slab.piece(stage)
        here = coordinate(me, axis)
        copies = []
        for d in range(1, size):
            there = lax.rem(here + d, size)
            if stage == 0:
                src = slab.src.at[rows_at(slab.row0 + there * piece, piece)]
            else:
                src = held[i].at[rows_at(offs[i] + there * piece, piece)]
            copies.append(send(src, land[4 * i + stage].at[d - 1], peer_of(me, axis, d)))
        pending[i] = copies

    def absorb(i, stage):
        slab = slabs[i]
        axis = slab.order[stage]
        piece = slab.piece(stage)
        here = coordinate(me, axis)
        for copy in pending[i]:
            copy.wait_recv()
        base = offs[i] + here * piece
        step = min(piece, 32)

        def add(k, _):
            at = k * step
            if stage == 0:
                total = slab.src[rows_at(slab.row0 + base + at, step), :]
            else:
                total = held[i][rows_at(base + at, step), :]
            for d in range(AXES[axis][0] - 1):
                total = total + land[4 * i + stage][d, rows_at(at, step), :]
            if stage == 0:
                held[i][rows_at(at, step), :] = total
            elif stage == 3:
                slab.dst[rows_at(slab.row0 + home[i] + at, step), :] = total
            else:
                held[i][rows_at(base + at, step), :] = total
            return 0

        if stage == 0:
            home[i] = here * piece
        else:
            home[i] = home[i] + here * piece
        lax.fori_loop(0, piece // step, add, 0)
        offs[i] = 0 if stage == 0 else base

    home = [0] * n

    for i in range(n):
        scatter(i, 0)
    for stage in range(4):
        for i in range(n):
            absorb(i, stage)
            if stage < 3:
                scatter(i, stage + 1)
            else:
                spread(i, 3, slabs, home, me, send, pending)
    for stage in (2, 1, 0):
        for i in range(n):
            for copy in pending[i]:
                copy.wait_recv()
            here = coordinate(me, slabs[i].order[stage + 1])
            home[i] = home[i] - here * slabs[i].piece(stage + 1)
            spread(i, stage, slabs, home, me, send, pending)
    for i in range(n):
        for copy in pending[i]:
            copy.wait_recv()
    for copy in started:
        copy.wait_send()


def spread(i, stage, slabs, home, me, send, pending):
    slab = slabs[i]
    axis = slab.order[stage]
    piece = slab.piece(stage)
    view = slab.dst.at[rows_at(slab.row0 + home[i], piece)]
    pending[i] = [send(view, view, peer_of(me, axis, d)) for d in range(1, AXES[axis][0])]


def sum_over_devices(dw_img, dw_txt, small, sub=2):
    plan = sum_plan(dw_img.shape[0], dw_txt.shape[0], sub)
    arrays = [dw_img, dw_txt, small]
    held, land = [], []
    copies = 0
    for a, _, rows, order in plan:
        width = arrays[a].shape[1]
        slab = Slab(None, None, 0, rows, order)
        held.append(pltpu.VMEM((slab.piece(0), width), jnp.float32))
        for stage in range(4):
            others = AXES[order[stage]][0] - 1
            land.append(pltpu.VMEM((others, slab.piece(stage), width), jnp.float32))
            copies += 2 * others
    return pl.pallas_call(
        functools.partial(sum_kernel, plan),
        out_shape=[jax.ShapeDtypeStruct(a.shape, jnp.float32) for a in arrays],
        in_specs=[pl.BlockSpec(memory_space=pltpu.VMEM)] * 3,
        out_specs=[pl.BlockSpec(memory_space=pltpu.VMEM)] * 3,
        scratch_shapes=held + land + [pltpu.SemaphoreType.DMA((copies,)), pltpu.SemaphoreType.DMA((copies,))],
        compiler_params=pltpu.CompilerParams(
            collective_id=1, has_side_effects=True, vmem_limit_bytes=60 * 1024 * 1024),
    )(*arrays)


ID_ROWS = 16
PIECES = {"T": 1, "I": 2}
SCHEDULE = (
    "RT00", "RI00", "RT10", "BT00", "RI01", "BI00", "BI01", "RI10",
    "I0b1", "I0n1", "RT20", "T2n1", "T1n0", "T0b1", "RI11", "BT10",
    "T0n0", "T1n1", "T1b1", "RI20", "BI10", "BT20", "T0n1", "T2b1",
    "RT30", "T2b0", "BI11", "RI21", "T1b0", "T3n1", "RI30", "I2n1",
    "BT30", "BI20", "I1b1", "T3b1", "BI21", "RI31", "SI", "I3n1",
    "I1n1", "BI30", "I2b1", "BI31", "I3b1", "ST", "I2b0", "T0b0",
    "T2n0", "I0b0", "I2n0", "I1n0", "T3n0", "I1b0", "I3b0", "I0n0",
    "I3n0", "T3b0",
)


def with_ids(block, ids):
    rows, width = block.shape
    digits = jnp.stack([lax.div(ids, 128), lax.rem(ids, 128)]).astype(jnp.bfloat16)
    digits = jnp.pad(digits, ((0, ID_ROWS - 2), (0, width - rows)))
    return jnp.concatenate([block, digits], axis=0)


def cross_kernel(scal_ref, img_in, txt_in, w_ref, img_out, txt_out, sums_ref,
                 img_all, txt_all, own_txt, emb, grad_ref, rid_img, rid_txt, acc_img, acc_txt, land_img, land_txt,
                 img_send, img_recv, txt_send, txt_recv, swap_send, swap_recv, copy_sem):
    rows = own_txt.shape[1]
    me = lax.axis_index("data")
    core, col_x, col_y, lev = (coordinate(me, a) for a in "cxyz")
    scale = scal_ref[0]
    bias = scal_ref[1]

    load_img = pltpu.make_async_copy(img_in, img_all.at[lev * 4 + col_x * 2 + core], copy_sem.at[0])
    load_txt = pltpu.make_async_copy(txt_in, txt_all.at[lev * 4 + col_y * 2 + core], copy_sem.at[1])
    load_img.start()
    load_txt.start()

    barrier = pltpu.get_barrier_semaphore()
    for axis in "cxy":
        pl.semaphore_signal(barrier, inc=1, device_id=(peer_of(me, axis, 1),), device_id_type=MESH_ID)

    @pl.when(lev > 0)
    def _():
        pl.semaphore_signal(barrier, inc=1, device_id=(me - 8,), device_id_type=MESH_ID)

    @pl.when(lev < 3)
    def _():
        pl.semaphore_signal(barrier, inc=1, device_id=(me + 8,), device_id_type=MESH_ID)

    pl.semaphore_wait(barrier, 3 + jnp.where(lev > 0, 1, 0) + jnp.where(lev < 3, 1, 0))

    class Stream:
        def __init__(self, kind, buf, send_sem, recv_sem, axis):
            self.pieces = PIECES[kind]
            self.buf, self.send_sem, self.recv_sem = buf, send_sem, recv_sem
            self.side = coordinate(me, axis)
            self.peers = (me + 8, me - 8, peer_of(me, axis, 1), peer_of(me, "c", 1))

        def slot(self, level, near, same_core):
            side = jnp.where(near, self.side, 1 - self.side)
            return level * 4 + side * 2 + jnp.where(same_core, core, 1 - core)

        def copy(self, slot, target, piece):
            share = rows // self.pieces
            size = share + (ID_ROWS if piece == self.pieces - 1 else 0)
            part = self.buf.at[slot, pl.ds(piece * share, size)]
            return pltpu.make_async_remote_copy(
                src_ref=part, dst_ref=part,
                send_sem=self.send_sem.at[(slot * 4 + target) * self.pieces + piece],
                recv_sem=self.recv_sem.at[slot * self.pieces + piece],
                device_id=(self.peers[target],), device_id_type=MESH_ID)

        def each_target(self, level, near, piece, act):
            slot = self.slot(level, near, True)
            if near:
                @pl.when((level <= lev) & (lev < 3))
                def _():
                    act(self.copy(slot, 0, piece))

                @pl.when((level >= lev) & (lev > 0))
                def _():
                    act(self.copy(slot, 1, piece))

                act(self.copy(slot, 2, piece))
            act(self.copy(slot, 3, piece))

        def arrive(self, level, near, same_core, piece):
            self.copy(self.slot(level, near, same_core), 3, piece).wait_recv()

        def relay(self, dist, near, piece):
            for sign in (-1, 1) if dist else (1,):
                level = lev + sign * dist

                @pl.when((level >= 0) & (level <= 3))
                def _():
                    if dist > 0 or not near:
                        self.arrive(level, near, True, piece)
                    self.each_target(level, near, piece, lambda c: c.start())

    txt = Stream("T", txt_all, txt_send, txt_recv, "y")
    img = Stream("I", img_all, img_send, img_recv, "x")
    streams = {"T": txt, "I": img}

    def swap(acc, land, axis, k):
        return pltpu.make_async_remote_copy(
            src_ref=acc.at[1], dst_ref=land, send_sem=swap_send.at[k], recv_sem=swap_recv.at[k],
            device_id=(peer_of(me, axis, 1),), device_id_type=MESH_ID)

    swaps = {"I": swap(acc_img, land_img, "x", 0), "T": swap(acc_txt, land_txt, "y", 1)}

    def level_at(k):
        inner = (lev == 1) | (lev == 2)
        near_low = jnp.where(inner & (k < 2), 1 - k, k)
        return jnp.where(lev >= 2, 3 - near_low, near_low)

    load_txt.wait()
    txt.relay(0, True, 0)
    load_img.wait()
    for piece in range(img.pieces):
        img.relay(0, True, piece)

    sums_ref[...] = jnp.zeros_like(sums_ref)
    acc_img[...] = jnp.zeros_like(acc_img)
    acc_txt[...] = jnp.zeros_like(acc_txt)

    def id_row(buf, slot):
        digits = buf[slot, pl.ds(rows, ID_ROWS), pl.ds(0, rows)].astype(jnp.float32)
        return digits[0:1] * 128.0 + digits[1:2]

    def id_tile(buf, slot):
        return jnp.transpose(jnp.broadcast_to(id_row(buf, slot), (COL_CHUNK, rows)))

    def embed_block(slot, dst):
        for cc in range(rows // COL_CHUNK):
            sl = pl.ds(cc * COL_CHUNK, COL_CHUNK)
            raw = jnp.dot(txt_all[slot, sl, :], w_ref[...], preferred_element_type=jnp.float32)
            inv = lax.rsqrt(jnp.sum(raw * raw, axis=1, keepdims=True))
            dst[sl, :] = (raw * inv).astype(jnp.bfloat16)

    def block_pass(row_view, rid, acc, half, col_views, cids, with_loss):
        for part in range(2):
            for cc in range(rows // COL_CHUNK):
                csl = pl.ds(cc * COL_CHUNK, COL_CHUNK)
                sim = lax.dot_general(row_view[pl.ds(0, rows), :], col_views[part][csl, :], CONTRACT_COLS,
                                      preferred_element_type=jnp.float32)
                match = rid[half] == cids[part][:, cc * COL_CHUNK:(cc + 1) * COL_CHUNK]
                margin = sim * scale + bias
                margin = jnp.where(match, -margin, margin)
                if with_loss:
                    expo = jnp.exp2(-jnp.abs(margin))
                    recip = 1.0 / (1.0 + expo)
                    sig = jnp.where(margin >= 0.0, recip, expo * recip)
                    grad = jnp.where(match, -sig, sig)
                    sums_ref[0] += fold_rows(jnp.maximum(margin, 0.0))
                    sums_ref[1] += log1p_sum(expo)
                    sums_ref[2] += fold_rows(grad * sim)
                    sums_ref[3] += fold_rows(grad)
                else:
                    sig = 1.0 / (1.0 + jnp.exp2(-margin))
                    grad = jnp.where(match, -sig, sig)
                grad_ref[:, pl.ds(part * rows + cc * COL_CHUNK, COL_CHUNK)] = grad.astype(jnp.bfloat16)
        total = jnp.dot(grad_ref[:, pl.ds(0, rows)], col_views[0][pl.ds(0, rows), :],
                        preferred_element_type=jnp.float32)
        total += jnp.dot(grad_ref[:, pl.ds(rows, rows)], col_views[1][pl.ds(0, rows), :],
                         preferred_element_type=jnp.float32)
        acc[half] += total

    def prepare():
        for half in range(2):
            slot = txt.slot(lev, half == 0, True)
            embed_block(slot, own_txt.at[half])
            rid_img[half] = id_tile(img_all, img.slot(lev, half == 0, True))
            rid_txt[half] = id_tile(txt_all, slot)

    before, codes, seen = [[]], [], set()
    for word in SCHEDULE:
        if word[0] in "RB":
            if word[0] == "B" or word[2] != "0":
                stream, dist, piece = streams[word[1]], int(word[2]), int(word[3])
                before[-1].append(functools.partial(stream.relay, dist, word[0] == "R", piece))
        elif word[0] == "S":
            before[-1].append(swaps[word[1]].start)
        else:
            kind, k, near, half = word[0], int(word[1]), word[2] == "n", int(word[3])
            if not codes:
                before[-1].append(prepare)
            if word[:3] not in seen:
                seen.add(word[:3])
                for piece in range(PIECES[kind]):
                    before[-1].append(functools.partial(
                        lambda st, k, near, piece: st.arrive(level_at(k), near, False, piece),
                        streams[kind], k, near, piece))
            codes.append((0 if kind == "T" else 16) + k * 4 + (0 if near else 2) + half)
            before.append([])

    def step(i, _):
        for at, acts in enumerate(before[:-1]):
            if acts:
                @pl.when(i == at)
                def _():
                    for act in acts:
                        act()

        code = jnp.int32(codes[0])
        for at in range(1, len(codes)):
            code = jnp.where(i == at, codes[at], code)
        half = lax.rem(code, 2)
        near = lax.rem(lax.div(code, 2), 2) == 0
        level = level_at(lax.rem(lax.div(code, 4), 4))

        @pl.when(code < 16)
        def _():
            slots = [txt.slot(level, near, same) for same in (True, False)]
            for part in range(2):
                embed_block(slots[part], emb.at[part])
            block_pass(img_all.at[img.slot(lev, half == 0, True)], rid_img, acc_img, half, [emb.at[0], emb.at[1]],
                       [id_row(txt_all, slot) for slot in slots], True)

        @pl.when(code >= 16)
        def _():
            slots = [img.slot(level, near, same) for same in (True, False)]
            block_pass(own_txt.at[half], rid_txt, acc_txt, half, [img_all.at[slot] for slot in slots],
                       [id_row(img_all, slot) for slot in slots], False)

        return 0

    lax.fori_loop(0, len(codes), step, 0)
    for act in before[-1]:
        act()

    def settle(level, _):
        for stream in (txt, img):
            for near in (True, False):
                for piece in range(stream.pieces):
                    stream.each_target(level, near, piece, lambda c: c.wait_send())
        return 0

    lax.fori_loop(0, 4, settle, 0)
    swaps["I"].wait()
    img_out[...] = acc_img[0] + land_img[...]
    swaps["T"].wait()
    txt_out[...] = acc_txt[0] + land_txt[...]


def cross_pass(scalars, img_block, txt_block, w_txt):
    rows, emb = img_block.shape[0] - ID_ROWS, img_block.shape[1]
    width = txt_block.shape[1]
    full = rows + ID_ROWS
    f32, bf16 = jnp.float32, jnp.bfloat16
    dma = pltpu.SemaphoreType.DMA
    return pl.pallas_call(
        cross_kernel,
        out_shape=[jax.ShapeDtypeStruct((rows, emb), f32), jax.ShapeDtypeStruct((rows, emb), f32),
                   jax.ShapeDtypeStruct((4, 8, COL_CHUNK), f32)],
        in_specs=[pl.BlockSpec(memory_space=pltpu.SMEM), pl.BlockSpec(memory_space=pl.ANY),
                  pl.BlockSpec(memory_space=pl.ANY), pl.BlockSpec(memory_space=pltpu.VMEM)],
        out_specs=[pl.BlockSpec(memory_space=pltpu.VMEM)] * 3,
        scratch_shapes=[
            pltpu.VMEM((16, full, emb), bf16), pltpu.VMEM((16, full, width), bf16),
            pltpu.VMEM((2, rows, emb), bf16), pltpu.VMEM((2, rows, emb), bf16), pltpu.VMEM((rows, 2 * rows), bf16),
            pltpu.VMEM((2, rows, COL_CHUNK), f32), pltpu.VMEM((2, rows, COL_CHUNK), f32),
            pltpu.VMEM((2, rows, emb), f32), pltpu.VMEM((2, rows, emb), f32),
            pltpu.VMEM((rows, emb), f32), pltpu.VMEM((rows, emb), f32),
            dma((64 * PIECES["I"],)), dma((16 * PIECES["I"],)), dma((64 * PIECES["T"],)), dma((16 * PIECES["T"],)), dma((2,)), dma((2,)), dma((2,)),
        ],
        compiler_params=pltpu.CompilerParams(
            collective_id=0, has_side_effects=True, vmem_limit_bytes=62 * 1024 * 1024),
    )(scalars, img_block, txt_block, w_txt)


def solution(mesh):
    n_dev = mesh.shape["data"]

    def local_fn(feat_img, feat_txt, w_img, w_txt, log_temp, logit_bias, pair_ids):
        total_rows = feat_img.shape[0] * n_dev
        temp_scale = jnp.exp(log_temp)
        scalars = jnp.stack([temp_scale * LOG2E, logit_bias * LOG2E])
        unit_img, inv_img, emb_img = embed_rows(feat_img, w_img)
        unit_txt, inv_txt, _ = embed_rows(feat_txt, w_txt)
        acc_img, acc_txt, sums = cross_pass(scalars, with_ids(emb_img, pair_ids), with_ids(feat_txt, pair_ids), w_txt)
        out_scale = temp_scale / total_rows
        dw_img = weight_grad(feat_img, unit_img, inv_img, out_scale * acc_img)
        dw_txt = weight_grad(feat_txt, unit_txt, inv_txt, out_scale * acc_txt)
        sums = jnp.sum(sums, axis=(1, 2))
        small = jnp.stack([LN2 * sums[0] + sums[1], sums[2], sums[3]]) / total_rows
        small = jnp.pad(small[:, None], ((0, 253), (0, 127)))
        dw_img, dw_txt, small = sum_over_devices(dw_img, dw_txt, small)
        return small[0, 0], temp_scale * small[1, 0], small[2, 0], dw_img, dw_txt

    return jax.shard_map(
        local_fn,
        mesh=mesh,
        in_specs=(P("data", None), P("data", None), P(None, None), P(None, None), P(), P(), P("data")),
        out_specs=(P(), P(), P(), P(None, None), P(None, None)),
        check_vma=False,
    )
```

```python
import functools

import jax
import jax.numpy as jnp
from jax import lax
from jax.experimental import pallas as pl
from jax.experimental.pallas import tpu as pltpu
from jax.sharding import PartitionSpec as P

CONTRACT_ROWS = (((0,), (0,)), ((), ()))
CONTRACT_COLS = (((1,), (1,)), ((), ()))
LOG2E = 1.4426950408889634
LN2 = 0.6931471805599453
COL_CHUNK = 256


def embed_rows(feat_rows, weights):
    raw_emb = jnp.dot(feat_rows, weights, preferred_element_type=jnp.float32)
    inv_norm = lax.rsqrt(jnp.sum(raw_emb * raw_emb, axis=1, keepdims=True))
    unit_emb = raw_emb * inv_norm
    return unit_emb, inv_norm, unit_emb.astype(jnp.bfloat16)


def weight_grad(feat_rows, unit_emb, inv_norm, grad_emb):
    raw_grad = inv_norm * (grad_emb - unit_emb * jnp.sum(unit_emb * grad_emb, axis=1, keepdims=True))
    return lax.dot_general(feat_rows, raw_grad.astype(jnp.bfloat16), CONTRACT_ROWS, preferred_element_type=jnp.float32)


def log1p_sum(expo):
    terms = [expo[8 * k:8 * k + 8] for k in range(expo.shape[0] // 8)]
    while len(terms) > 1:
        terms = [terms[2 * k] + terms[2 * k + 1] + terms[2 * k] * terms[2 * k + 1] for k in range(len(terms) // 2)]
    prod = terms[0]
    one_plus = 1.0 + prod
    return jnp.log(one_plus) + (prod - (one_plus - 1.0)) / one_plus


def fold_rows(tile):
    terms = [tile[8 * k:8 * k + 8] for k in range(tile.shape[0] // 8)]
    while len(terms) > 1:
        terms = [terms[2 * k] + terms[2 * k + 1] for k in range(len(terms) // 2)]
    return terms[0]


AXES = {"c": (2, 1), "x": (2, 2), "y": (2, 4), "u": (2, 8), "v": (2, 16), "z": (4, 8)}
MESH_ID = pl.DeviceIdType.MESH
UNIT = 256
SUM_ORDERS = ("cyuvx", "cxyuv", "cuxyv", "cxyuv", "cxyvu", "cxyuv", "cyxuv", "cuyxv", "cyuxv", "cxyuv")
SUM_STEPS = (
    0, 10, 50, 70, 80, 30, 11, 1, 20, 51, 12, 90, 100, 81, 31, 71, 21, 52, 13, 32,
    82, 60, 2, 40, 33, 14, 34, 83, 41, 72, 15, 61, 53, 22, 35, 84, 42, 91, 101, 16,
    23, 36, 62, 3, 85, 54, 73, 92, 102, 24, 17, 43, 4, 63, 55, 93, 103, 44, 74, 86,
    64, 25, 37, 56, 45, 94, 104, 75, 87, 5, 65, 26, 46, 38, 57, 76, 95, 105, 6, 66,
    27, 96, 106, 47, 7, 67, 97, 107, 77, 88, 28, 18, 58, 48, 49, 29, 8, 89, 59, 78,
    98, 108, 39, 9, 68, 19, 99, 109, 69, 79,
)


def coordinate(me, axis):
    size, stride = AXES[axis]
    return lax.rem(lax.div(me, stride), size)


def peer_of(me, axis, dist=1):
    size, stride = AXES[axis]
    here = coordinate(me, axis)
    return me + (lax.rem(here + dist, size) - here) * stride


def rows_at(start, size):
    return pl.ds(pl.multiple_of(start, 8), size)


def sum_kernel(orders, steps, *refs):
    ins, outs = refs[:3], refs[3:6]
    n = len(orders)
    held = refs[6:6 + n]
    land = refs[6 + n:6 + 6 * n]
    send_sem, recv_sem = refs[6 + 6 * n:]
    me = lax.axis_index("data")
    bits = {axis: coordinate(me, axis) for axis in "cxyuv"}
    peers = {axis: peer_of(me, axis) for axis in "cxyuv"}
    img_units = ins[0].shape[0] // UNIT
    txt_units = ins[1].shape[0] // UNIT
    place = [(0, u * UNIT) for u in range(img_units)] + [(1, u * UNIT) for u in range(txt_units)] + [(2, 0)]

    barrier = pltpu.get_barrier_semaphore()
    for axis in "cxyuv":
        pl.semaphore_signal(barrier, inc=1, device_id=(peers[axis],), device_id_type=MESH_ID)
    pl.semaphore_wait(barrier, 5)

    base = [0] * n
    home = [0] * n
    pending = [None] * n
    started = []

    def send(i, stage, src, dst):
        k = len(started)
        pending[i] = pltpu.make_async_remote_copy(
            src_ref=src, dst_ref=dst, send_sem=send_sem.at[k], recv_sem=recv_sem.at[k],
            device_id=(peers[orders[i][stage]],), device_id_type=MESH_ID)
        pending[i].start()
        started.append(pending[i])

    def scatter(i, stage):
        size = UNIT >> (stage + 1)
        other = (1 - bits[orders[i][stage]]) * size
        array, row0 = place[i]
        src = ins[array].at[rows_at(row0 + other, size)] if stage == 0 else held[i].at[rows_at(base[i] + other, size)]
        send(i, stage, src, land[5 * i + stage])

    def spread(i, stage):
        array, row0 = place[i]
        view = outs[array].at[rows_at(row0 + home[i], UNIT >> (stage + 1))]
        send(i, stage, view, view)

    def absorb(i, stage):
        pending[i].wait_recv()
        size = UNIT >> (stage + 1)
        array, row0 = place[i]
        mine = bits[orders[i][stage]] * size
        home[i] = home[i] + mine
        step = min(size, 32)

        def add(k, _):
            at = k * step
            part = land[5 * i + stage][rows_at(at, step), :]
            if stage == 0:
                held[i][rows_at(at, step), :] = ins[array][rows_at(row0 + mine + at, step), :] + part
            elif stage == 4:
                outs[array][rows_at(row0 + home[i] + at, step), :] = held[i][rows_at(base[i] + mine + at, step), :] + part
            else:
                held[i][rows_at(base[i] + mine + at, step), :] += part
            return 0

        lax.fori_loop(0, size // step, add, 0)
        base[i] = 0 if stage == 0 else base[i] + mine

    for i in range(n):
        scatter(i, 0)
    for code in steps:
        i, stage = divmod(code, 10)
        if stage < 5:
            absorb(i, stage)
            if stage < 4:
                scatter(i, stage + 1)
            else:
                spread(i, 4)
        else:
            pending[i].wait_recv()
            left = 9 - stage
            home[i] = home[i] - bits[orders[i][left]] * (UNIT >> (left + 1))
            if left > 0:
                spread(i, left - 1)
    for copy in started:
        copy.wait_send()


def sum_over_devices(dw_img, dw_txt, small):
    arrays = [dw_img, dw_txt, small]
    orders = SUM_ORDERS + (SUM_ORDERS[-1],)
    widths = [dw_img.shape[1]] * len(SUM_ORDERS) + [small.shape[1]]
    held = [pltpu.VMEM((UNIT // 2, width), jnp.float32) for width in widths]
    land = [pltpu.VMEM((UNIT >> (stage + 1), width), jnp.float32) for width in widths for stage in range(5)]
    copies = 10 * len(orders)
    return pl.pallas_call(
        functools.partial(sum_kernel, orders, SUM_STEPS),
        out_shape=[jax.ShapeDtypeStruct(a.shape, jnp.float32) for a in arrays],
        in_specs=[pl.BlockSpec(memory_space=pltpu.VMEM)] * 3,
        out_specs=[pl.BlockSpec(memory_space=pltpu.VMEM)] * 3,
        scratch_shapes=held + land + [pltpu.SemaphoreType.DMA((copies,)), pltpu.SemaphoreType.DMA((copies,))],
        compiler_params=pltpu.CompilerParams(
            collective_id=1, has_side_effects=True, vmem_limit_bytes=60 * 1024 * 1024),
    )(*arrays)


ID_ROWS = 16
PIECES = {"T": 1, "I": 2}
SCHEDULE = (
    "RT00", "RI00", "RT10", "BT00", "RI01", "BI00", "BI01", "RI10",
    "I0b1", "I0n1", "RT20", "T2n1", "T1n0", "T0b1", "RI11", "BT10",
    "T0n0", "T1n1", "T1b1", "RI20", "BI10", "BT20", "T0n1", "T2b1",
    "RT30", "T2b0", "BI11", "RI21", "T1b0", "T3n1", "RI30", "I2n1",
    "BT30", "BI20", "I1b1", "T3b1", "BI21", "RI31", "SI", "I3n1",
    "I1n1", "BI30", "I2b1", "BI31", "I3b1", "ST", "I2b0", "T0b0",
    "T2n0", "I0b0", "I2n0", "I1n0", "T3n0", "I1b0", "I3b0", "I0n0",
    "I3n0", "T3b0",
)


def with_ids(block, ids):
    rows, width = block.shape
    digits = jnp.stack([lax.div(ids, 128), lax.rem(ids, 128)]).astype(jnp.bfloat16)
    digits = jnp.pad(digits, ((0, ID_ROWS - 2), (0, width - rows)))
    return jnp.concatenate([block, digits], axis=0)


def cross_kernel(scal_ref, img_in, txt_in, w_ref, img_out, txt_out, sums_ref,
                 img_all, txt_all, own_txt, emb, grad_ref, rid_img, rid_txt, acc_img, acc_txt, land_img, land_txt,
                 img_send, img_recv, txt_send, txt_recv, swap_send, swap_recv, copy_sem):
    rows = own_txt.shape[1]
    me = lax.axis_index("data")
    core, col_x, col_y, lev = (coordinate(me, a) for a in "cxyz")
    scale = scal_ref[0]
    bias = scal_ref[1]

    load_img = pltpu.make_async_copy(img_in, img_all.at[lev * 4 + col_x * 2 + core], copy_sem.at[0])
    load_txt = pltpu.make_async_copy(txt_in, txt_all.at[lev * 4 + col_y * 2 + core], copy_sem.at[1])
    load_img.start()
    load_txt.start()

    barrier = pltpu.get_barrier_semaphore()
    for axis in "cxy":
        pl.semaphore_signal(barrier, inc=1, device_id=(peer_of(me, axis, 1),), device_id_type=MESH_ID)

    @pl.when(lev > 0)
    def _():
        pl.semaphore_signal(barrier, inc=1, device_id=(me - 8,), device_id_type=MESH_ID)

    @pl.when(lev < 3)
    def _():
        pl.semaphore_signal(barrier, inc=1, device_id=(me + 8,), device_id_type=MESH_ID)

    pl.semaphore_wait(barrier, 3 + jnp.where(lev > 0, 1, 0) + jnp.where(lev < 3, 1, 0))

    class Stream:
        def __init__(self, kind, buf, send_sem, recv_sem, axis):
            self.pieces = PIECES[kind]
            self.buf, self.send_sem, self.recv_sem = buf, send_sem, recv_sem
            self.side = coordinate(me, axis)
            self.peers = (me + 8, me - 8, peer_of(me, axis, 1), peer_of(me, "c", 1))

        def slot(self, level, near, same_core):
            side = jnp.where(near, self.side, 1 - self.side)
            return level * 4 + side * 2 + jnp.where(same_core, core, 1 - core)

        def copy(self, slot, target, piece):
            share = rows // self.pieces
            size = share + (ID_ROWS if piece == self.pieces - 1 else 0)
            part = self.buf.at[slot, pl.ds(piece * share, size)]
            return pltpu.make_async_remote_copy(
                src_ref=part, dst_ref=part,
                send_sem=self.send_sem.at[(slot * 4 + target) * self.pieces + piece],
                recv_sem=self.recv_sem.at[slot * self.pieces + piece],
                device_id=(self.peers[target],), device_id_type=MESH_ID)

        def each_target(self, level, near, piece, act):
            slot = self.slot(level, near, True)
            if near:
                @pl.when((level <= lev) & (lev < 3))
                def _():
                    act(self.copy(slot, 0, piece))

                @pl.when((level >= lev) & (lev > 0))
                def _():
                    act(self.copy(slot, 1, piece))

                act(self.copy(slot, 2, piece))
            act(self.copy(slot, 3, piece))

        def arrive(self, level, near, same_core, piece):
            self.copy(self.slot(level, near, same_core), 3, piece).wait_recv()

        def relay(self, dist, near, piece):
            for sign in (-1, 1) if dist else (1,):
                level = lev + sign * dist

                @pl.when((level >= 0) & (level <= 3))
                def _():
                    if dist > 0 or not near:
                        self.arrive(level, near, True, piece)
                    self.each_target(level, near, piece, lambda c: c.start())

    txt = Stream("T", txt_all, txt_send, txt_recv, "y")
    img = Stream("I", img_all, img_send, img_recv, "x")
    streams = {"T": txt, "I": img}

    def swap(acc, land, axis, k):
        return pltpu.make_async_remote_copy(
            src_ref=acc.at[1], dst_ref=land, send_sem=swap_send.at[k], recv_sem=swap_recv.at[k],
            device_id=(peer_of(me, axis, 1),), device_id_type=MESH_ID)

    swaps = {"I": swap(acc_img, land_img, "x", 0), "T": swap(acc_txt, land_txt, "y", 1)}

    def level_at(k):
        inner = (lev == 1) | (lev == 2)
        near_low = jnp.where(inner & (k < 2), 1 - k, k)
        return jnp.where(lev >= 2, 3 - near_low, near_low)

    load_txt.wait()
    txt.relay(0, True, 0)
    load_img.wait()
    for piece in range(img.pieces):
        img.relay(0, True, piece)

    sums_ref[...] = jnp.zeros_like(sums_ref)
    acc_img[...] = jnp.zeros_like(acc_img)
    acc_txt[...] = jnp.zeros_like(acc_txt)

    def id_row(buf, slot):
        digits = buf[slot, pl.ds(rows, ID_ROWS), pl.ds(0, rows)].astype(jnp.float32)
        return digits[0:1] * 128.0 + digits[1:2]

    def id_tile(buf, slot):
        return jnp.transpose(jnp.broadcast_to(id_row(buf, slot), (COL_CHUNK, rows)))

    def embed_block(slot, dst):
        for cc in range(rows // COL_CHUNK):
            sl = pl.ds(cc * COL_CHUNK, COL_CHUNK)
            raw = jnp.dot(txt_all[slot, sl, :], w_ref[...], preferred_element_type=jnp.float32)
            inv = lax.rsqrt(jnp.sum(raw * raw, axis=1, keepdims=True))
            dst[sl, :] = (raw * inv).astype(jnp.bfloat16)

    def block_pass(row_view, rid, acc, half, col_views, cids, with_loss):
        for part in range(2):
            for cc in range(rows // COL_CHUNK):
                csl = pl.ds(cc * COL_CHUNK, COL_CHUNK)
                sim = lax.dot_general(row_view[pl.ds(0, rows), :], col_views[part][csl, :], CONTRACT_COLS,
                                      preferred_element_type=jnp.float32)
                match = rid[half] == cids[part][:, cc * COL_CHUNK:(cc + 1) * COL_CHUNK]
                margin = sim * scale + bias
                margin = jnp.where(match, -margin, margin)
                if with_loss:
                    expo = jnp.exp2(-jnp.abs(margin))
                    recip = 1.0 / (1.0 + expo)
                    sig = jnp.where(margin >= 0.0, recip, expo * recip)
                    grad = jnp.where(match, -sig, sig)
                    sums_ref[0] += fold_rows(jnp.maximum(margin, 0.0))
                    sums_ref[1] += log1p_sum(expo)
                    sums_ref[2] += fold_rows(grad * sim)
                    sums_ref[3] += fold_rows(grad)
                else:
                    sig = 1.0 / (1.0 + jnp.exp2(-margin))
                    grad = jnp.where(match, -sig, sig)
                grad_ref[:, pl.ds(part * rows + cc * COL_CHUNK, COL_CHUNK)] = grad.astype(jnp.bfloat16)
        total = jnp.dot(grad_ref[:, pl.ds(0, rows)], col_views[0][pl.ds(0, rows), :],
                        preferred_element_type=jnp.float32)
        total += jnp.dot(grad_ref[:, pl.ds(rows, rows)], col_views[1][pl.ds(0, rows), :],
                         preferred_element_type=jnp.float32)
        acc[half] += total

    def prepare():
        for half in range(2):
            slot = txt.slot(lev, half == 0, True)
            embed_block(slot, own_txt.at[half])
            rid_img[half] = id_tile(img_all, img.slot(lev, half == 0, True))
            rid_txt[half] = id_tile(txt_all, slot)

    before, codes, seen = [[]], [], set()
    for word in SCHEDULE:
        if word[0] in "RB":
            if word[0] == "B" or word[2] != "0":
                stream, dist, piece = streams[word[1]], int(word[2]), int(word[3])
                before[-1].append(functools.partial(stream.relay, dist, word[0] == "R", piece))
        elif word[0] == "S":
            before[-1].append(swaps[word[1]].start)
        else:
            kind, k, near, half = word[0], int(word[1]), word[2] == "n", int(word[3])
            if not codes:
                before[-1].append(prepare)
            if word[:3] not in seen:
                seen.add(word[:3])
                for piece in range(PIECES[kind]):
                    before[-1].append(functools.partial(
                        lambda st, k, near, piece: st.arrive(level_at(k), near, False, piece),
                        streams[kind], k, near, piece))
            codes.append((0 if kind == "T" else 16) + k * 4 + (0 if near else 2) + half)
            before.append([])

    def step(i, _):
        for at, acts in enumerate(before[:-1]):
            if acts:
                @pl.when(i == at)
                def _():
                    for act in acts:
                        act()

        code = jnp.int32(codes[0])
        for at in range(1, len(codes)):
            code = jnp.where(i == at, codes[at], code)
        half = lax.rem(code, 2)
        near = lax.rem(lax.div(code, 2), 2) == 0
        level = level_at(lax.rem(lax.div(code, 4), 4))

        @pl.when(code < 16)
        def _():
            slots = [txt.slot(level, near, same) for same in (True, False)]
            for part in range(2):
                embed_block(slots[part], emb.at[part])
            block_pass(img_all.at[img.slot(lev, half == 0, True)], rid_img, acc_img, half, [emb.at[0], emb.at[1]],
                       [id_row(txt_all, slot) for slot in slots], True)

        @pl.when(code >= 16)
        def _():
            slots = [img.slot(level, near, same) for same in (True, False)]
            block_pass(own_txt.at[half], rid_txt, acc_txt, half, [img_all.at[slot] for slot in slots],
                       [id_row(img_all, slot) for slot in slots], False)

        return 0

    lax.fori_loop(0, len(codes), step, 0)
    for act in before[-1]:
        act()

    def settle(level, _):
        for stream in (txt, img):
            for near in (True, False):
                for piece in range(stream.pieces):
                    stream.each_target(level, near, piece, lambda c: c.wait_send())
        return 0

    lax.fori_loop(0, 4, settle, 0)
    swaps["I"].wait()
    img_out[...] = acc_img[0] + land_img[...]
    swaps["T"].wait()
    txt_out[...] = acc_txt[0] + land_txt[...]


def cross_pass(scalars, img_block, txt_block, w_txt):
    rows, emb = img_block.shape[0] - ID_ROWS, img_block.shape[1]
    width = txt_block.shape[1]
    full = rows + ID_ROWS
    f32, bf16 = jnp.float32, jnp.bfloat16
    dma = pltpu.SemaphoreType.DMA
    return pl.pallas_call(
        cross_kernel,
        out_shape=[jax.ShapeDtypeStruct((rows, emb), f32), jax.ShapeDtypeStruct((rows, emb), f32),
                   jax.ShapeDtypeStruct((4, 8, COL_CHUNK), f32)],
        in_specs=[pl.BlockSpec(memory_space=pltpu.SMEM), pl.BlockSpec(memory_space=pl.ANY),
                  pl.BlockSpec(memory_space=pl.ANY), pl.BlockSpec(memory_space=pltpu.VMEM)],
        out_specs=[pl.BlockSpec(memory_space=pltpu.VMEM)] * 3,
        scratch_shapes=[
            pltpu.VMEM((16, full, emb), bf16), pltpu.VMEM((16, full, width), bf16),
            pltpu.VMEM((2, rows, emb), bf16), pltpu.VMEM((2, rows, emb), bf16), pltpu.VMEM((rows, 2 * rows), bf16),
            pltpu.VMEM((2, rows, COL_CHUNK), f32), pltpu.VMEM((2, rows, COL_CHUNK), f32),
            pltpu.VMEM((2, rows, emb), f32), pltpu.VMEM((2, rows, emb), f32),
            pltpu.VMEM((rows, emb), f32), pltpu.VMEM((rows, emb), f32),
            dma((64 * PIECES["I"],)), dma((16 * PIECES["I"],)), dma((64 * PIECES["T"],)), dma((16 * PIECES["T"],)), dma((2,)), dma((2,)), dma((2,)),
        ],
        compiler_params=pltpu.CompilerParams(
            collective_id=0, has_side_effects=True, vmem_limit_bytes=62 * 1024 * 1024),
    )(scalars, img_block, txt_block, w_txt)


def solution(mesh):
    n_dev = mesh.shape["data"]

    def local_fn(feat_img, feat_txt, w_img, w_txt, log_temp, logit_bias, pair_ids):
        total_rows = feat_img.shape[0] * n_dev
        temp_scale = jnp.exp(log_temp)
        scalars = jnp.stack([temp_scale * LOG2E, logit_bias * LOG2E])
        unit_img, inv_img, emb_img = embed_rows(feat_img, w_img)
        unit_txt, inv_txt, _ = embed_rows(feat_txt, w_txt)
        acc_img, acc_txt, sums = cross_pass(scalars, with_ids(emb_img, pair_ids), with_ids(feat_txt, pair_ids), w_txt)
        out_scale = temp_scale / total_rows
        dw_img = weight_grad(feat_img, unit_img, inv_img, out_scale * acc_img)
        dw_txt = weight_grad(feat_txt, unit_txt, inv_txt, out_scale * acc_txt)
        sums = jnp.sum(sums, axis=(1, 2))
        small = jnp.stack([LN2 * sums[0] + sums[1], sums[2], sums[3]]) / total_rows
        small = jnp.pad(small[:, None], ((0, 253), (0, 127)))
        dw_img, dw_txt, small = sum_over_devices(dw_img, dw_txt, small)
        return small[0, 0], temp_scale * small[1, 0], small[2, 0], dw_img, dw_txt

    return jax.shard_map(
        local_fn,
        mesh=mesh,
        in_specs=(P("data", None), P("data", None), P(None, None), P(None, None), P(), P(), P("data")),
        out_specs=(P(), P(), P(), P(None, None), P(None, None)),
        check_vma=False,
    )
```

```python
import functools

import jax
import jax.numpy as jnp
from jax import lax
from jax.experimental import pallas as pl
from jax.experimental.pallas import tpu as pltpu
from jax.sharding import PartitionSpec as P

CONTRACT_ROWS = (((0,), (0,)), ((), ()))
CONTRACT_COLS = (((1,), (1,)), ((), ()))
LOG2E = 1.4426950408889634
LN2 = 0.6931471805599453
COL_CHUNK = 256


def embed_rows(feat_rows, weights):
    raw_emb = jnp.dot(feat_rows, weights, preferred_element_type=jnp.float32)
    inv_norm = lax.rsqrt(jnp.sum(raw_emb * raw_emb, axis=1, keepdims=True))
    unit_emb = raw_emb * inv_norm
    return unit_emb, inv_norm, unit_emb.astype(jnp.bfloat16)


def raw_grad(unit_emb, inv_norm, grad_emb):
    grad = inv_norm * (grad_emb - unit_emb * jnp.sum(unit_emb * grad_emb, axis=1, keepdims=True))
    return grad.astype(jnp.bfloat16)


def log1p_sum(expo):
    terms = [expo[8 * k:8 * k + 8] for k in range(expo.shape[0] // 8)]
    while len(terms) > 1:
        terms = [terms[2 * k] + terms[2 * k + 1] + terms[2 * k] * terms[2 * k + 1] for k in range(len(terms) // 2)]
    prod = terms[0]
    one_plus = 1.0 + prod
    return jnp.log(one_plus) + (prod - (one_plus - 1.0)) / one_plus


def fold_rows(tile):
    terms = [tile[8 * k:8 * k + 8] for k in range(tile.shape[0] // 8)]
    while len(terms) > 1:
        terms = [terms[2 * k] + terms[2 * k + 1] for k in range(len(terms) // 2)]
    return terms[0]


AXES = {"c": (2, 1), "x": (2, 2), "y": (2, 4), "u": (2, 8), "v": (2, 16), "z": (4, 8)}
MESH_ID = pl.DeviceIdType.MESH
UNIT = 256
SUM_ORDERS = ("cyuvx", "cxyuv", "cuxyv", "cxyuv", "cxyvu", "cxyuv", "cyxuv", "cuyxv", "cyuxv", "cxyuv")
SUM_STEPS = (
    0, 10, 50, 70, 80, 30, 11, 1, 20, 51, 12, 90, 100, 81, 31, 71, 21, 52, 13, 32,
    82, 60, 2, 40, 33, 14, 34, 83, 41, 72, 15, 61, 53, 22, 35, 84, 42, 91, 101, 16,
    23, 36, 62, 3, 85, 54, 73, 92, 102, 24, 17, 43, 4, 63, 55, 93, 103, 44, 74, 86,
    64, 25, 37, 56, 45, 94, 104, 75, 87, 5, 65, 26, 46, 38, 57, 76, 95, 105, 6, 66,
    27, 96, 106, 47, 7, 67, 97, 107, 77, 88, 28, 18, 58, 48, 49, 29, 8, 89, 59, 78,
    98, 108, 39, 9, 68, 19, 99, 109, 69, 79,
)


def coordinate(me, axis):
    size, stride = AXES[axis]
    return lax.rem(lax.div(me, stride), size)


def peer_of(me, axis, dist=1):
    size, stride = AXES[axis]
    here = coordinate(me, axis)
    return me + (lax.rem(here + dist, size) - here) * stride


def rows_at(start, size):
    return pl.ds(pl.multiple_of(start, 8), size)


def sum_kernel(orders, steps, *refs):
    n = len(orders)
    feats, grads, outs = refs[0:2], refs[2:4], refs[5:8]
    ins = (refs[8], refs[9], refs[4])
    held = refs[10:10 + n]
    land = refs[10 + n:10 + 6 * n]
    send_sem, recv_sem = refs[10 + 6 * n:]
    me = lax.axis_index("data")
    bits = {axis: coordinate(me, axis) for axis in "cxyuv"}
    peers = {axis: peer_of(me, axis) for axis in "cxyuv"}
    img_units = outs[0].shape[0] // UNIT
    txt_units = outs[1].shape[0] // UNIT
    place = [(0, u * UNIT) for u in range(img_units)] + [(1, u * UNIT) for u in range(txt_units)] + [(2, 0)]

    barrier = pltpu.get_barrier_semaphore()
    for axis in "cxyuv":
        pl.semaphore_signal(barrier, inc=1, device_id=(peers[axis],), device_id_type=MESH_ID)
    pl.semaphore_wait(barrier, 5)

    base = [0] * n
    home = [0] * n
    pending = [None] * n
    started = []

    def send(i, stage, src, dst):
        k = len(started)
        pending[i] = pltpu.make_async_remote_copy(
            src_ref=src, dst_ref=dst, send_sem=send_sem.at[k], recv_sem=recv_sem.at[k],
            device_id=(peers[orders[i][stage]],), device_id_type=MESH_ID)
        pending[i].start()
        started.append(pending[i])

    def scatter(i, stage):
        size = UNIT >> (stage + 1)
        other = (1 - bits[orders[i][stage]]) * size
        array, row0 = place[i]
        src = ins[array].at[rows_at(row0 + other, size)] if stage == 0 else held[i].at[rows_at(base[i] + other, size)]
        send(i, stage, src, land[5 * i + stage])

    def spread(i, stage):
        array, row0 = place[i]
        view = outs[array].at[rows_at(row0 + home[i], UNIT >> (stage + 1))]
        send(i, stage, view, view)

    def absorb(i, stage):
        pending[i].wait_recv()
        size = UNIT >> (stage + 1)
        array, row0 = place[i]
        mine = bits[orders[i][stage]] * size
        home[i] = home[i] + mine
        step = min(size, 32)

        def add(k, _):
            at = k * step
            part = land[5 * i + stage][rows_at(at, step), :]
            if stage == 0:
                held[i][rows_at(at, step), :] = ins[array][rows_at(row0 + mine + at, step), :] + part
            elif stage == 4:
                outs[array][rows_at(row0 + home[i] + at, step), :] = held[i][rows_at(base[i] + mine + at, step), :] + part
            else:
                held[i][rows_at(base[i] + mine + at, step), :] += part
            return 0

        lax.fori_loop(0, size // step, add, 0)
        base[i] = 0 if stage == 0 else base[i] + mine

    for i in range(n):
        array, row0 = place[i]
        if array < 2:
            ins[array][pl.ds(row0, UNIT), :] = lax.dot_general(
                feats[array][:, pl.ds(row0, UNIT)], grads[array][...], CONTRACT_ROWS,
                preferred_element_type=jnp.float32)
        scatter(i, 0)
    for code in steps:
        i, stage = divmod(code, 10)
        if stage < 5:
            absorb(i, stage)
            if stage < 4:
                scatter(i, stage + 1)
            else:
                spread(i, 4)
        else:
            pending[i].wait_recv()
            left = 9 - stage
            home[i] = home[i] - bits[orders[i][left]] * (UNIT >> (left + 1))
            if left > 0:
                spread(i, left - 1)
    for copy in started:
        copy.wait_send()


def sum_over_devices(feats, grads, small):
    emb = grads[0].shape[1]
    shapes = [(feat.shape[1], emb) for feat in feats] + [small.shape]
    orders = SUM_ORDERS + (SUM_ORDERS[-1],)
    widths = [emb] * len(SUM_ORDERS) + [small.shape[1]]
    held = [pltpu.VMEM((UNIT // 2, width), jnp.float32) for width in widths]
    land = [pltpu.VMEM((UNIT >> (stage + 1), width), jnp.float32) for width in widths for stage in range(5)]
    copies = 10 * len(orders)
    return pl.pallas_call(
        functools.partial(sum_kernel, orders, SUM_STEPS),
        out_shape=[jax.ShapeDtypeStruct(shape, jnp.float32) for shape in shapes],
        in_specs=[pl.BlockSpec(memory_space=pltpu.VMEM)] * 5,
        out_specs=[pl.BlockSpec(memory_space=pltpu.VMEM)] * 3,
        scratch_shapes=[pltpu.VMEM(shape, jnp.float32) for shape in shapes[:2]] + held + land + [pltpu.SemaphoreType.DMA((copies,)), pltpu.SemaphoreType.DMA((copies,))],
        compiler_params=pltpu.CompilerParams(
            collective_id=1, has_side_effects=True, vmem_limit_bytes=60 * 1024 * 1024),
    )(*feats, *grads, small)


ID_ROWS = 16
PIECES = {"T": 1, "I": 2}
SCHEDULE = (
    "RT00", "RI00", "RT10", "BT00", "RI01", "BI00", "BI01", "RI10",
    "I0b1", "I0n1", "RT20", "T2n1", "T1n0", "T0b1", "RI11", "BT10",
    "T0n0", "T1n1", "T1b1", "RI20", "BI10", "BT20", "T0n1", "T2b1",
    "RT30", "T2b0", "BI11", "RI21", "T1b0", "T3n1", "RI30", "I2n1",
    "BT30", "BI20", "I1b1", "T3b1", "BI21", "RI31", "SI", "I3n1",
    "I1n1", "BI30", "I2b1", "BI31", "I3b1", "ST", "I2b0", "T0b0",
    "T2n0", "I0b0", "I2n0", "I1n0", "T3n0", "I1b0", "I3b0", "I0n0",
    "I3n0", "T3b0",
)


def with_ids(block, ids):
    rows, width = block.shape
    digits = jnp.stack([lax.div(ids, 128), lax.rem(ids, 128)]).astype(jnp.bfloat16)
    digits = jnp.pad(digits, ((0, ID_ROWS - 2), (0, width - rows)))
    return jnp.concatenate([block, digits], axis=0)


def cross_kernel(scal_ref, img_in, txt_in, w_ref, img_out, txt_out, sums_ref,
                 img_all, txt_all, own_txt, emb, grad_ref, rid_img, rid_txt, acc_img, acc_txt, land_img, land_txt,
                 img_send, img_recv, txt_send, txt_recv, swap_send, swap_recv, copy_sem):
    rows = own_txt.shape[1]
    me = lax.axis_index("data")
    core, col_x, col_y, lev = (coordinate(me, a) for a in "cxyz")
    scale = scal_ref[0]
    bias = scal_ref[1]

    load_img = pltpu.make_async_copy(img_in, img_all.at[lev * 4 + col_x * 2 + core], copy_sem.at[0])
    load_txt = pltpu.make_async_copy(txt_in, txt_all.at[lev * 4 + col_y * 2 + core], copy_sem.at[1])
    load_img.start()
    load_txt.start()

    barrier = pltpu.get_barrier_semaphore()
    for axis in "cxy":
        pl.semaphore_signal(barrier, inc=1, device_id=(peer_of(me, axis, 1),), device_id_type=MESH_ID)

    @pl.when(lev > 0)
    def _():
        pl.semaphore_signal(barrier, inc=1, device_id=(me - 8,), device_id_type=MESH_ID)

    @pl.when(lev < 3)
    def _():
        pl.semaphore_signal(barrier, inc=1, device_id=(me + 8,), device_id_type=MESH_ID)

    pl.semaphore_wait(barrier, 3 + jnp.where(lev > 0, 1, 0) + jnp.where(lev < 3, 1, 0))

    class Stream:
        def __init__(self, kind, buf, send_sem, recv_sem, axis):
            self.pieces = PIECES[kind]
            self.buf, self.send_sem, self.recv_sem = buf, send_sem, recv_sem
            self.side = coordinate(me, axis)
            self.peers = (me + 8, me - 8, peer_of(me, axis, 1), peer_of(me, "c", 1))

        def slot(self, level, near, same_core):
            side = jnp.where(near, self.side, 1 - self.side)
            return level * 4 + side * 2 + jnp.where(same_core, core, 1 - core)

        def copy(self, slot, target, piece):
            share = rows // self.pieces
            size = share + (ID_ROWS if piece == self.pieces - 1 else 0)
            part = self.buf.at[slot, pl.ds(piece * share, size)]
            return pltpu.make_async_remote_copy(
                src_ref=part, dst_ref=part,
                send_sem=self.send_sem.at[(slot * 4 + target) * self.pieces + piece],
                recv_sem=self.recv_sem.at[slot * self.pieces + piece],
                device_id=(self.peers[target],), device_id_type=MESH_ID)

        def each_target(self, level, near, piece, act):
            slot = self.slot(level, near, True)
            if near:
                @pl.when((level <= lev) & (lev < 3))
                def _():
                    act(self.copy(slot, 0, piece))

                @pl.when((level >= lev) & (lev > 0))
                def _():
                    act(self.copy(slot, 1, piece))

                act(self.copy(slot, 2, piece))
            act(self.copy(slot, 3, piece))

        def arrive(self, level, near, same_core, piece):
            self.copy(self.slot(level, near, same_core), 3, piece).wait_recv()

        def relay(self, dist, near, piece):
            for sign in (-1, 1) if dist else (1,):
                level = lev + sign * dist

                @pl.when((level >= 0) & (level <= 3))
                def _():
                    if dist > 0 or not near:
                        self.arrive(level, near, True, piece)
                    self.each_target(level, near, piece, lambda c: c.start())

    txt = Stream("T", txt_all, txt_send, txt_recv, "y")
    img = Stream("I", img_all, img_send, img_recv, "x")
    streams = {"T": txt, "I": img}

    def swap(acc, land, axis, k):
        return pltpu.make_async_remote_copy(
            src_ref=acc.at[1], dst_ref=land, send_sem=swap_send.at[k], recv_sem=swap_recv.at[k],
            device_id=(peer_of(me, axis, 1),), device_id_type=MESH_ID)

    swaps = {"I": swap(acc_img, land_img, "x", 0), "T": swap(acc_txt, land_txt, "y", 1)}

    def level_at(k):
        inner = (lev == 1) | (lev == 2)
        near_low = jnp.where(inner & (k < 2), 1 - k, k)
        return jnp.where(lev >= 2, 3 - near_low, near_low)

    load_txt.wait()
    txt.relay(0, True, 0)
    load_img.wait()
    for piece in range(img.pieces):
        img.relay(0, True, piece)

    sums_ref[...] = jnp.zeros_like(sums_ref)
    acc_img[...] = jnp.zeros_like(acc_img)
    acc_txt[...] = jnp.zeros_like(acc_txt)

    def id_row(buf, slot):
        digits = buf[slot, pl.ds(rows, ID_ROWS), pl.ds(0, rows)].astype(jnp.float32)
        return digits[0:1] * 128.0 + digits[1:2]

    def id_tile(buf, slot):
        return jnp.transpose(jnp.broadcast_to(id_row(buf, slot), (COL_CHUNK, rows)))

    def embed_block(slot, dst):
        for cc in range(rows // COL_CHUNK):
            sl = pl.ds(cc * COL_CHUNK, COL_CHUNK)
            raw = jnp.dot(txt_all[slot, sl, :], w_ref[...], preferred_element_type=jnp.float32)
            inv = lax.rsqrt(jnp.sum(raw * raw, axis=1, keepdims=True))
            dst[sl, :] = (raw * inv).astype(jnp.bfloat16)

    def block_pass(row_view, rid, acc, half, col_views, cids, with_loss):
        for part in range(2):
            for cc in range(rows // COL_CHUNK):
                csl = pl.ds(cc * COL_CHUNK, COL_CHUNK)
                sim = lax.dot_general(row_view[pl.ds(0, rows), :], col_views[part][csl, :], CONTRACT_COLS,
                                      preferred_element_type=jnp.float32)
                match = rid[half] == cids[part][:, cc * COL_CHUNK:(cc + 1) * COL_CHUNK]
                margin = sim * scale + bias
                margin = jnp.where(match, -margin, margin)
                if with_loss:
                    expo = jnp.exp2(-jnp.abs(margin))
                    recip = 1.0 / (1.0 + expo)
                    sig = jnp.where(margin >= 0.0, recip, expo * recip)
                    grad = jnp.where(match, -sig, sig)
                    sums_ref[0] += fold_rows(jnp.maximum(margin, 0.0))
                    sums_ref[1] += log1p_sum(expo)
                    sums_ref[2] += fold_rows(grad * sim)
                    sums_ref[3] += fold_rows(grad)
                else:
                    sig = 1.0 / (1.0 + jnp.exp2(-margin))
                    grad = jnp.where(match, -sig, sig)
                grad_ref[:, pl.ds(part * rows + cc * COL_CHUNK, COL_CHUNK)] = grad.astype(jnp.bfloat16)
        total = jnp.dot(grad_ref[:, pl.ds(0, rows)], col_views[0][pl.ds(0, rows), :],
                        preferred_element_type=jnp.float32)
        total += jnp.dot(grad_ref[:, pl.ds(rows, rows)], col_views[1][pl.ds(0, rows), :],
                         preferred_element_type=jnp.float32)
        acc[half] += total

    def prepare():
        for half in range(2):
            slot = txt.slot(lev, half == 0, True)
            embed_block(slot, own_txt.at[half])
            rid_img[half] = id_tile(img_all, img.slot(lev, half == 0, True))
            rid_txt[half] = id_tile(txt_all, slot)

    before, codes, seen = [[]], [], set()
    for word in SCHEDULE:
        if word[0] in "RB":
            if word[0] == "B" or word[2] != "0":
                stream, dist, piece = streams[word[1]], int(word[2]), int(word[3])
                before[-1].append(functools.partial(stream.relay, dist, word[0] == "R", piece))
        elif word[0] == "S":
            before[-1].append(swaps[word[1]].start)
        else:
            kind, k, near, half = word[0], int(word[1]), word[2] == "n", int(word[3])
            if not codes:
                before[-1].append(prepare)
            if word[:3] not in seen:
                seen.add(word[:3])
                for piece in range(PIECES[kind]):
                    before[-1].append(functools.partial(
                        lambda st, k, near, piece: st.arrive(level_at(k), near, False, piece),
                        streams[kind], k, near, piece))
            codes.append((0 if kind == "T" else 16) + k * 4 + (0 if near else 2) + half)
            before.append([])

    def step(i, _):
        for at, acts in enumerate(before[:-1]):
            if acts:
                @pl.when(i == at)
                def _():
                    for act in acts:
                        act()

        code = jnp.int32(codes[0])
        for at in range(1, len(codes)):
            code = jnp.where(i == at, codes[at], code)
        half = lax.rem(code, 2)
        near = lax.rem(lax.div(code, 2), 2) == 0
        level = level_at(lax.rem(lax.div(code, 4), 4))

        @pl.when(code < 16)
        def _():
            slots = [txt.slot(level, near, same) for same in (True, False)]
            for part in range(2):
                embed_block(slots[part], emb.at[part])
            block_pass(img_all.at[img.slot(lev, half == 0, True)], rid_img, acc_img, half, [emb.at[0], emb.at[1]],
                       [id_row(txt_all, slot) for slot in slots], True)

        @pl.when(code >= 16)
        def _():
            slots = [img.slot(level, near, same) for same in (True, False)]
            block_pass(own_txt.at[half], rid_txt, acc_txt, half, [img_all.at[slot] for slot in slots],
                       [id_row(img_all, slot) for slot in slots], False)

        return 0

    lax.fori_loop(0, len(codes), step, 0)
    for act in before[-1]:
        act()

    def settle(level, _):
        for stream in (txt, img):
            for near in (True, False):
                for piece in range(stream.pieces):
                    stream.each_target(level, near, piece, lambda c: c.wait_send())
        return 0

    lax.fori_loop(0, 4, settle, 0)
    swaps["I"].wait()
    img_out[...] = acc_img[0] + land_img[...]
    swaps["T"].wait()
    txt_out[...] = acc_txt[0] + land_txt[...]


def cross_pass(scalars, img_block, txt_block, w_txt):
    rows, emb = img_block.shape[0] - ID_ROWS, img_block.shape[1]
    width = txt_block.shape[1]
    full = rows + ID_ROWS
    f32, bf16 = jnp.float32, jnp.bfloat16
    dma = pltpu.SemaphoreType.DMA
    return pl.pallas_call(
        cross_kernel,
        out_shape=[jax.ShapeDtypeStruct((rows, emb), f32), jax.ShapeDtypeStruct((rows, emb), f32),
                   jax.ShapeDtypeStruct((4, 8, COL_CHUNK), f32)],
        in_specs=[pl.BlockSpec(memory_space=pltpu.SMEM), pl.BlockSpec(memory_space=pl.ANY),
                  pl.BlockSpec(memory_space=pl.ANY), pl.BlockSpec(memory_space=pltpu.VMEM)],
        out_specs=[pl.BlockSpec(memory_space=pltpu.VMEM)] * 3,
        scratch_shapes=[
            pltpu.VMEM((16, full, emb), bf16), pltpu.VMEM((16, full, width), bf16),
            pltpu.VMEM((2, rows, emb), bf16), pltpu.VMEM((2, rows, emb), bf16), pltpu.VMEM((rows, 2 * rows), bf16),
            pltpu.VMEM((2, rows, COL_CHUNK), f32), pltpu.VMEM((2, rows, COL_CHUNK), f32),
            pltpu.VMEM((2, rows, emb), f32), pltpu.VMEM((2, rows, emb), f32),
            pltpu.VMEM((rows, emb), f32), pltpu.VMEM((rows, emb), f32),
            dma((64 * PIECES["I"],)), dma((16 * PIECES["I"],)), dma((64 * PIECES["T"],)), dma((16 * PIECES["T"],)), dma((2,)), dma((2,)), dma((2,)),
        ],
        compiler_params=pltpu.CompilerParams(
            collective_id=0, has_side_effects=True, vmem_limit_bytes=62 * 1024 * 1024),
    )(scalars, img_block, txt_block, w_txt)


def solution(mesh):
    n_dev = mesh.shape["data"]

    def local_fn(feat_img, feat_txt, w_img, w_txt, log_temp, logit_bias, pair_ids):
        total_rows = feat_img.shape[0] * n_dev
        temp_scale = jnp.exp(log_temp)
        scalars = jnp.stack([temp_scale * LOG2E, logit_bias * LOG2E])
        unit_img, inv_img, emb_img = embed_rows(feat_img, w_img)
        unit_txt, inv_txt, _ = embed_rows(feat_txt, w_txt)
        acc_img, acc_txt, sums = cross_pass(scalars, with_ids(emb_img, pair_ids), with_ids(feat_txt, pair_ids), w_txt)
        out_scale = temp_scale / total_rows
        grad_img = raw_grad(unit_img, inv_img, out_scale * acc_img)
        grad_txt = raw_grad(unit_txt, inv_txt, out_scale * acc_txt)
        sums = jnp.sum(sums, axis=(1, 2))
        small = jnp.stack([LN2 * sums[0] + sums[1], sums[2], sums[3]]) / total_rows
        small = jnp.pad(small[:, None], ((0, 253), (0, 127)))
        dw_img, dw_txt, small = sum_over_devices((feat_img, feat_txt), (grad_img, grad_txt), small)
        return small[0, 0], temp_scale * small[1, 0], small[2, 0], dw_img, dw_txt

    return jax.shard_map(
        local_fn,
        mesh=mesh,
        in_specs=(P("data", None), P("data", None), P(None, None), P(None, None), P(), P(), P("data")),
        out_specs=(P(), P(), P(), P(None, None), P(None, None)),
        check_vma=False,
    )
```
